32 devices in a mesh: batch: 4 (over y, x), seq: 8 (over z, core), section: 1.
Axes of the slice: x: 2, y: 2, z: 4, core: 2. Of those that a mesh axis runs over, the one named last changes fastest.
Arguments:
- acts: bfloat16 [1, 14848, 5120], P('section', ('batch', 'seq')), may hold values from -13 to 13
- cotangent: float32 [1, 14848, 6], P('section', ('batch', 'seq')), may hold values from -120 to 120
- routes: int32 [1, 14848, 6], P('section', ('batch', 'seq')), may hold values from 0 to 159, all different within a row
- router_weight: bfloat16 [1, 5120, 160], P('section', ('batch', 'seq')), may hold values from -0.078125 to 0.078125
Outputs:
- grad_router: float32 [1, 5120, 160], P('section', ('batch', 'seq'))
The draws below stay inside these ranges and needn't reach their ends.
Inputs may be any that keep to these rules, and one draw needn't show every extreme that they name: `routes`: each token's row names 6 different experts, and every expert is named by some token.
All inputs are finite; a program needn't handle non-finite values.
Results may differ from the reference program's by a relative error of at most 0.0017.
Values may be sent and summed in bfloat16 or wider, within the bound.
A program may use at most 64 MiB of HBM per device.

```python
import math
import jax
import jax.numpy as jnp
from jax import lax

D = 5120
EXPERTS = 160
TOPK = 6
TOK_DEV = 464
LAYERS = 1
TOKENS = 14848


def draw_acts(key, part):
    groups = TOKENS // TOK_DEV
    block_width = D // groups
    base_key = jax.random.fold_in(key, 11)
    offset_key = jax.random.fold_in(key, 12)
    pair_key = jax.random.fold_in(key, 13)
    base = jnp.clip(jax.random.normal(base_key, (LAYERS, TOKENS, D), jnp.float32), -4.0, 4.0)
    pairing = jax.random.permutation(pair_key, groups)
    token_group = jnp.arange(TOKENS, dtype=jnp.int32) // TOK_DEV
    feature_group = jnp.arange(D, dtype=jnp.int32) // block_width
    paired = pairing[token_group][:, None] == feature_group[None, :]
    spike = jnp.where(paired, 3.0, 1.0).astype(jnp.float32)
    offset = 0.12 * jnp.clip(jax.random.normal(offset_key, (LAYERS, 1, D), jnp.float32), -3.0, 3.0)
    values = base * spike[None, :, :] + offset
    return values.astype(jnp.bfloat16)


def draw_cotangent(key, part):
    base = jnp.clip(jax.random.normal(key, (LAYERS, TOKENS, TOPK), jnp.float32) + 1.5, -4.0, 4.0)
    span = 4.0
    position = jnp.arange(TOKENS, dtype=jnp.float32) / TOKENS
    row_scale = jnp.exp(jnp.log(span) * position)
    layer_scale = 1.0 + 2.0 * jnp.arange(LAYERS, dtype=jnp.float32) / max(LAYERS - 1, 1)
    values = base * row_scale[None, :, None] * layer_scale[:, None, None]
    return values.astype(jnp.float32)


def block_levels(rng, dims, cuts, low, largest):
    factor_of = 1.0
    for dim, parts in cuts:
        heights = jax.random.uniform(jax.random.fold_in(jax.random.fold_in(rng, 6), dim), (parts,), jnp.float32, low / len(cuts), largest / len(cuts))
        factor_of = factor_of * jnp.repeat(jnp.exp(heights), dims[dim] // parts).reshape((-1,) + (1,) * (len(dims) - 1 - dim))
    return factor_of


def different_ones(rng, rows, number_of, top, lift):
    sequence = jax.random.permutation(jax.random.fold_in(rng, 1), number_of)
    favour = sequence
    for power in range(3):
        favour = favour * favour // number_of
    favour = favour * lift // number_of
    chance = jax.random.randint(jax.random.fold_in(rng, 2), (rows, number_of), 0, 4096) + favour
    fixed_rows = jax.random.permutation(jax.random.fold_in(rng, 3), rows)[jnp.arange(number_of) % rows]
    chance = jnp.where(jnp.arange(rows)[:, None] == fixed_rows[None, :], 1 << 14, chance)
    merit = chance * number_of + jnp.arange(number_of)
    return lax.top_k(merit.astype(jnp.int32), top)[1].astype(jnp.int32)


def bell_draw(key, extent, scale, most, pieces=(), held_as=jnp.bfloat16):
    factor_of = block_levels(key, extent, pieces, -0.22, 0.18) if pieces else 1.0
    array = jax.random.normal(key, extent, jnp.float32) * scale * factor_of
    return jnp.minimum(jnp.maximum(array, -most), most).astype(held_as)


def setup_inputs(seed: int = 0) -> dict:
    arg_keys = jax.random.split(jax.random.key(seed), 5)
    return {
        "acts": draw_acts(jax.random.fold_in(arg_keys[4], 71), 0),
        "cotangent": draw_cotangent(jax.random.fold_in(arg_keys[4], 71), 0),
        "routes": different_ones(arg_keys[2], LAYERS * TOKENS, EXPERTS, TOPK, 307).reshape((LAYERS, TOKENS, TOPK)),
        "router_weight": bell_draw(arg_keys[3], (LAYERS, D, EXPERTS), D ** -0.5, 0.078125, ((1, 32),)),
    }


def over_tokens(left, right):
    return lax.dot_general(left, right, (((0,), (0,)), ((), ())), preferred_element_type=jnp.float32)

def layer_grad(x_layer, cot_layer, route_layer, weight_layer):
    logits = jnp.dot(x_layer, weight_layer, preferred_element_type=jnp.float32)
    expo = jnp.exp(logits)
    probs = expo / lax.optimization_barrier(jnp.sum(expo, axis=-1, keepdims=True))
    expert_ids = jnp.arange(EXPERTS, dtype=jnp.int32)
    picks = (route_layer[:, :, None] == expert_ids[None, None, :]).astype(jnp.float32)
    d_prob = lax.optimization_barrier(jnp.sum(cot_layer[:, :, None] * picks, axis=1))
    inner = lax.optimization_barrier(jnp.sum(probs * d_prob, axis=-1, keepdims=True))
    d_logits = (probs * (d_prob - inner)).astype(jnp.bfloat16)
    return over_tokens(x_layer, d_logits)

def reference(acts, cotangent, routes, router_weight):
    raw = []
    for layer in range(LAYERS):
        raw.append(layer_grad(acts[layer], cotangent[layer], routes[layer], router_weight[layer]))
    raw = jnp.stack(raw)
    square_sum = jnp.sum(raw * raw)
    clip_norm = 0.25 * math.sqrt(1.0 * LAYERS * D * EXPERTS)
    clip_scale = jnp.minimum(jnp.float32(1.0), clip_norm / jnp.sqrt(square_sum))
    return raw * clip_scale
```

```python
import functools
import math

import jax
import jax.numpy as jnp
from jax import lax
from jax.experimental import pallas as pl
from jax.experimental.pallas import tpu as pltpu
from jax.sharding import PartitionSpec as P

MESH = pl.DeviceIdType.MESH
LANES = 128


def shards(acts, cotangent, routes, router_weight):
    layers = acts.shape[0]
    width = acts.shape[2]
    experts = router_weight.shape[2]
    logits = jnp.einsum(
        "ltd,lde->lte",
        acts,
        lax.all_gather(router_weight, ("batch", "seq"), axis=1, tiled=True),
        preferred_element_type=jnp.float32,
    )
    expo = jnp.exp(logits)
    probs = expo / jnp.sum(expo, axis=-1, keepdims=True)
    expert_ids = jnp.arange(experts, dtype=jnp.int32)
    picks = (routes[:, :, :, None] == expert_ids[None, None, None, :]).astype(jnp.float32)
    d_prob = jnp.sum(cotangent[:, :, :, None] * picks, axis=2)
    inner = jnp.sum(probs * d_prob, axis=-1, keepdims=True)
    d_logits = (probs * (d_prob - inner)).astype(jnp.bfloat16)
    batch_rows = lax.psum_scatter(
        jnp.einsum("ltd,lte->dle", acts, d_logits, preferred_element_type=jnp.float32),
        "batch",
        scatter_dimension=0,
        tiled=True,
    )
    summed = lax.psum_scatter(batch_rows, "seq", scatter_dimension=0, tiled=True)
    summed = jnp.transpose(summed, (1, 0, 2))
    square_sum = lax.psum(jnp.sum(summed * summed), ("batch", "seq", "section"))
    entry_count = 1.0 * layers * lax.axis_size("section") * width * experts
    clip_norm = 0.25 * math.sqrt(entry_count)
    clip_scale = jnp.minimum(jnp.float32(1.0), clip_norm / jnp.sqrt(square_sum))
    return summed * clip_scale


def kernel(cfg, acts_hbm, cot_ref, routes_ref, w_ref, out_ref,
           acts_v, wq, wg, logit, dprob, dt, part, rec_c, rec_f, rec_s, rec_l, rec_h,
           quad, flip, sq,
           acts_sem, q_send, q_recv, ag_send, ag_recv, fw_send, fw_recv,
           rs_send, rs_recv, fin_send, fin_recv, sq_send, sq_recv):
    n_batch, n_seq, tokens, width, experts, rows, chunks, clip_norm = cfg
    n_dev = n_batch * n_seq
    quad_cols = 4 * rows
    tail = experts - LANES
    half, quarter = experts // 2, experts // 4
    hrow = rows // 2
    b, s = lax.axis_index("batch"), lax.axis_index("seq")
    y, x = b // 2, b % 2
    z, c = s // 2, s % 2
    zh, zl = z // 2, z % 2
    me = b * n_seq + s
    p_own = zl * 2 + c

    def dev(dy=0, dx=0, dh=0, dl=0, dc=0):
        bb = ((y + dy) % 2) * 2 + (x + dx) % 2
        ss = (((zh + dh) % 2) * 2 + (zl + dl) % 2) * 2 + (c + dc) % 2
        return (bb, ss, 0)

    core, near, far = dev(dc=1), dev(dl=1), dev(dh=1)
    first = dev(dx=1 - c, dy=c)
    second = dev(dx=c, dy=1 - c)

    barrier = pltpu.get_barrier_semaphore()
    for d in range(1, n_dev):
        t = (me + d) % n_dev
        pl.semaphore_signal(barrier, inc=1, device_id=(t // n_seq, t % n_seq, 0), device_id_type=MESH)
    load = pltpu.make_async_copy(acts_hbm, acts_v, acts_sem)
    load.start()
    pl.semaphore_wait(barrier, n_dev - 1)

    sends = []

    def remote(src, dst, ssem, rsem, target):
        copy = pltpu.make_async_remote_copy(
            src_ref=src, dst_ref=dst, send_sem=ssem, recv_sem=rsem,
            device_id=target, device_id_type=MESH)
        copy.start()
        sends.append(copy)
        return copy

    to_core = remote(w_ref, wq.at[p_own], q_send.at[0], q_recv.at[0], core)
    to_near = remote(w_ref, wq.at[p_own], q_send.at[1], q_recv.at[1], near)
    wq[p_own] = w_ref[...]

    lane = lax.broadcasted_iota(jnp.int32, (tokens, 2 * LANES), 1)
    total = jnp.zeros((tokens, 2 * LANES), jnp.float32)
    for k in range(cot_ref.shape[1]):
        total += jnp.where(routes_ref[:, k:k + 1] == lane, cot_ref[:, k:k + 1], 0.0)
    dprob[...] = total

    to_near.wait_recv()
    p_near = (1 - zl) * 2 + c
    relay = remote(wq.at[p_near], wq.at[p_near], q_send.at[2], q_recv.at[2], core)
    to_core.wait_recv()
    relay.wait_recv()

    def slot(df, ds, dz):
        yy = (y + df * c + ds * (1 - c)) % 2
        xx = (x + df * (1 - c) + ds * c) % 2
        return yy * 4 + xx * 2 + (zh + dz) % 2

    own = slot(0, 0, 0)
    for h in range(2):
        rng = slice(h * hrow, (h + 1) * hrow)
        for p in range(4):
            wg[own, h, p] = wq[p, rng, :LANES]
        wg[own, h, 4] = jnp.concatenate([wq[p, rng, LANES:] for p in range(4)], axis=1)

    def ag(src, dst, target):
        at = slot(*src)
        i = dst[0] * 4 + dst[1] * 2 + dst[2]
        return remote(wg.at[at, c], wg.at[at, c], ag_send.at[i], ag_recv.at[i], target)

    def fw(src):
        at = slot(*src)
        i = src[0] * 4 + src[1] * 2 + src[2]
        return remote(wg.at[at, c], wg.at[at, c], fw_send.at[i], fw_recv.at[i], core)

    seg = lax.broadcasted_iota(jnp.int32, (rows, LANES), 1) // tail

    def add_logits(src, fresh=False):
        g = slot(*src)
        a_part = jnp.concatenate([wg[g, h, p] for p in range(4) for h in range(2)], axis=0)
        packed = jnp.concatenate([wg[g, 0, 4], wg[g, 1, 4]], axis=0)
        b_part = jnp.concatenate(
            [jnp.where(seg == p, packed, jnp.zeros_like(packed)) for p in range(4)], axis=0)
        w_part = jnp.concatenate([a_part, b_part], axis=1)
        cols = pl.ds(pl.multiple_of(g * quad_cols, LANES), quad_cols)
        term = jnp.dot(acts_v[:, cols], w_part, preferred_element_type=jnp.float32)
        if fresh:
            logit[...] = term
        else:
            logit[...] += term

    c001 = ag((0, 0, 0), (0, 0, 1), far)
    c100 = ag((0, 0, 0), (1, 0, 0), first)
    c010 = ag((0, 0, 0), (0, 1, 0), second)
    load.wait()
    add_logits((0, 0, 0), fresh=True)
    c100.wait_recv()
    c110 = ag((1, 0, 0), (1, 1, 0), second)
    f100 = fw((1, 0, 0))
    c010.wait_recv()
    f010 = fw((0, 1, 0))
    f100.wait_recv()
    add_logits((0, 1, 0))
    f010.wait_recv()
    add_logits((1, 0, 0))
    c001.wait_recv()
    c101 = ag((0, 0, 1), (1, 0, 1), first)
    c011 = ag((0, 0, 1), (0, 1, 1), second)
    f001 = fw((0, 0, 1))
    c110.wait_recv()
    f110 = fw((1, 1, 0))
    f001.wait_recv()
    add_logits((0, 0, 1))
    f110.wait_recv()
    add_logits((1, 1, 0))
    c101.wait_recv()
    c111 = ag((1, 0, 1), (1, 1, 1), second)
    f101 = fw((1, 0, 1))
    c011.wait_recv()
    f011 = fw((0, 1, 1))
    f101.wait_recv()
    add_logits((0, 1, 1))
    f011.wait_recv()
    add_logits((1, 0, 1))
    c111.wait_recv()
    f111 = fw((1, 1, 1))
    f111.wait_recv()
    add_logits((1, 1, 1))

    tl = logit[:, LANES:]
    folded = tl
    for r in range(1, 4):
        folded = folded + pltpu.roll(tl, r * tail, 1)
    expo_a = jnp.exp(logit[:, :LANES])
    expo_b = jnp.where(lane[:, :LANES] < tail, jnp.exp(folded), 0.0)
    norm = jnp.sum(expo_a + expo_b, axis=1, keepdims=True)
    prob_a, prob_b = expo_a / norm, expo_b / norm
    dp_a, dp_b = dprob[:, :LANES], dprob[:, LANES:]
    inner = jnp.sum(prob_a * dp_a + prob_b * dp_b, axis=1, keepdims=True)
    pad = jnp.zeros((flip.shape[0] - tokens, LANES), jnp.float32)
    for i, value in enumerate((prob_a * (dp_a - inner), prob_b * (dp_b - inner))):
        turned = jnp.transpose(jnp.concatenate([value, pad], axis=0))
        n = LANES if i == 0 else tail
        dt[i * LANES:i * LANES + n, :] = turned[:n, :tokens].astype(jnp.bfloat16)

    def compute(k0, nk):
        for g in range(8):
            gy, gx, gz = g // 4, g // 2 % 2, g % 2
            at = g * quad_cols + k0 * LANES
            value = jnp.dot(dt[...], acts_v[:, at:at + nk * LANES], preferred_element_type=jnp.float32)
            for kk in range(nk):
                for h in range(2):
                    f, e = (gx, gy) if h == 0 else (gy, gx)
                    for q in range(2):
                        r = h * half + q * quarter
                        part[k0 + kk, h, f, e, gz, q] = value[r:r + quarter, kk * LANES:(kk + 1) * LANES]

    fi = x * (1 - c) + y * c
    si = y * (1 - c) + x * c
    n_chunks = len(chunks)

    def rs_start(stage, i):
        k0, nk = chunks[i]
        ks = pl.ds(k0, nk)
        src, dst, target = [
            lambda: (part.at[ks, 1 - c], rec_c.at[ks], core),
            lambda: (part.at[ks, c, 1 - fi], rec_f.at[ks], first),
            lambda: (part.at[ks, c, fi, 1 - si], rec_s.at[ks], second),
            lambda: (part.at[ks, c, fi, si, :, 1 - zl], rec_l.at[ks], near),
            lambda: (part.at[ks, c, fi, si, 1 - zh, zl], rec_h.at[ks], far),
        ][stage]()
        n = stage * n_chunks + i
        return remote(src, dst, rs_send.at[n], rs_recv.at[n], target)

    def rs_finish(stage, i, copy):
        copy.wait_recv()
        k0, nk = chunks[i]
        for k in range(k0, k0 + nk):
            if stage == 0:
                part[k, c] += rec_c[k]
            elif stage == 1:
                part[k, c, fi] += rec_f[k]
            elif stage == 2:
                part[k, c, fi, si] += rec_s[k]
            elif stage == 3:
                for q in range(2):
                    part[k, c, fi, si, q, zl] += rec_l[k, q]
            else:
                part[k, c, fi, si, zh, zl] += rec_h[k]

    flying = {}
    for i in range(n_chunks):
        compute(*chunks[i])
        flying[0, i] = rs_start(0, i)
        if i > 0:
            rs_finish(0, i - 1, flying[0, i - 1])
            flying[1, i - 1] = rs_start(1, i - 1)
    rs_finish(0, n_chunks - 1, flying[0, n_chunks - 1])
    flying[1, n_chunks - 1] = rs_start(1, n_chunks - 1)
    for wave in range(n_chunks + 3):
        for stage in (1, 2, 3, 4):
            i = wave - (stage - 1)
            if 0 <= i < n_chunks:
                rs_finish(stage, i, flying[stage, i])
                if stage < 4:
                    flying[stage + 1, i] = rs_start(stage + 1, i)

    squares = jnp.zeros((quarter, LANES), jnp.float32)
    for k in range(quad_cols // LANES):
        v = part[k, c, fi, si, zh, zl]
        rec_h[k] = v
        squares += v * v
    sq[me] = jnp.broadcast_to(jnp.sum(squares).reshape(1, 1), (1, LANES))
    sq_copies = []
    for d in range(1, n_dev):
        t = (me + d) % n_dev
        sq_copies.append(pltpu.make_async_remote_copy(
            src_ref=sq.at[me], dst_ref=sq.at[me], send_sem=sq_send.at[d], recv_sem=sq_recv.at[d],
            device_id=(t // n_seq, t % n_seq, 0), device_id_type=MESH))
        sq_copies[-1].start()
    q_own = c * 2 + zl
    fins = []
    for n, (dl, dc) in enumerate(((1, 0), (1, 1), (0, 1))):
        p_to = ((zl + dl) % 2) * 2 + (c + dc) % 2
        fins.append(remote(rec_h.at[pl.ds(p_to, 2)], quad.at[q_own], fin_send.at[n], fin_recv.at[n],
                           dev(dl=dl, dc=dc)))
    quad[q_own] = rec_h[pl.ds(p_own, 2)]
    for copy in fins:
        copy.wait_recv()
    for j in range(2):
        block = jnp.concatenate([quad[q, j] for q in range(4)]
                                + [jnp.zeros((2 * LANES - experts, LANES), jnp.float32)], axis=0)
        flip[j * LANES:(j + 1) * LANES, :] = jnp.transpose(block)
    for copy in sq_copies:
        copy.wait()
    total_sq = jnp.sum(jnp.sum(sq[...], axis=0)) * (1.0 / LANES)
    clip_scale = jnp.minimum(jnp.float32(1.0), clip_norm / jnp.sqrt(jnp.full((1, 1), total_sq, jnp.float32)))
    mine = flip[pl.ds(pl.multiple_of(p_own * (rows - LANES), 8), rows), :]
    out_ref[...] = mine[:, :experts] * clip_scale
    for copy in sends:
        copy.wait_send()


def fused(mesh, acts, cotangent, routes, router_weight):
    n_batch, n_seq = mesh.shape["batch"], mesh.shape["seq"]
    layers, tokens, width = acts.shape
    rows, experts = router_weight.shape[1:]
    topk = routes.shape[2]
    quad_tiles = 4 * rows // LANES
    quarter = experts // 4
    chunks = tuple((k, min(2, quad_tiles - k)) for k in range(0, quad_tiles, 2))
    clip_norm = 0.25 * math.sqrt(1.0 * layers * width * experts)
    cfg = (n_batch, n_seq, tokens, width, experts, rows, chunks, clip_norm)
    f32, bf16 = jnp.float32, jnp.bfloat16
    dma = pltpu.SemaphoreType.DMA
    vmem = pl.BlockSpec(memory_space=pltpu.VMEM)
    padded = -(-tokens // LANES) * LANES
    n_dev = n_batch * n_seq
    n_rs = 5 * len(chunks)
    out = pl.pallas_call(
        functools.partial(kernel, cfg),
        out_shape=jax.ShapeDtypeStruct((rows, experts), f32),
        in_specs=[pl.BlockSpec(memory_space=pl.ANY), vmem, vmem, vmem],
        out_specs=vmem,
        scratch_shapes=[
            pltpu.VMEM((tokens, width), bf16),
            pltpu.VMEM((4, rows, experts), bf16),
            pltpu.VMEM((8, 2, 5, rows // 2, LANES), bf16),
            pltpu.VMEM((tokens, 2 * LANES), f32),
            pltpu.VMEM((tokens, 2 * LANES), f32),
            pltpu.VMEM((experts, tokens), bf16),
            pltpu.VMEM((quad_tiles, 2, 2, 2, 2, 2, quarter, LANES), f32),
            pltpu.VMEM((quad_tiles, 2, 2, 2, 2, quarter, LANES), f32),
            pltpu.VMEM((quad_tiles, 2, 2, 2, quarter, LANES), f32),
            pltpu.VMEM((quad_tiles, 2, 2, quarter, LANES), f32),
            pltpu.VMEM((quad_tiles, 2, quarter, LANES), f32),
            pltpu.VMEM((quad_tiles, quarter, LANES), f32),
            pltpu.VMEM((4, 2, quarter, LANES), f32),
            pltpu.VMEM((padded, 2 * LANES), f32),
            pltpu.VMEM((n_dev, 1, LANES), f32),
            dma, dma((3,)), dma((3,)), dma((8,)), dma((8,)), dma((8,)), dma((8,)),
            dma((n_rs,)), dma((n_rs,)), dma((3,)), dma((3,)), dma((n_dev,)), dma((n_dev,)),
        ],
        compiler_params=pltpu.CompilerParams(
            collective_id=0, has_side_effects=True, vmem_limit_bytes=48 * 1024 * 1024),
        name="router_grad",
    )(acts[0], cotangent[0], routes[0], router_weight[0])
    return out[None]


def solution(mesh):
    spec = P("section", ("batch", "seq"), None)

    def step(acts, cotangent, routes, router_weight):
        rows, experts = router_weight.shape[1:]
        cube = (mesh.shape["batch"], mesh.shape["seq"], mesh.shape["section"]) == (4, 8, 1)
        dense = (acts.shape[0] == 1 and LANES < experts == rows and 4 * (experts - LANES) == LANES
                 and 4 * rows == 5 * LANES and acts.shape[1] % 16 == 0)
        if cube and dense:
            return fused(mesh, acts, cotangent, routes, router_weight)
        return shards(acts, cotangent, routes, router_weight)

    return jax.shard_map(step, mesh=mesh, in_specs=(spec,) * 4, out_specs=spec, check_vma=False)
```

```python
import functools
import math

import jax
import jax.numpy as jnp
from jax import lax
from jax.experimental import pallas as pl
from jax.experimental.pallas import tpu as pltpu
from jax.sharding import PartitionSpec as P

MESH = pl.DeviceIdType.MESH
LANES = 128


def shards(acts, cotangent, routes, router_weight):
    layers = acts.shape[0]
    width = acts.shape[2]
    experts = router_weight.shape[2]
    logits = jnp.einsum(
        "ltd,lde->lte",
        acts,
        lax.all_gather(router_weight, ("batch", "seq"), axis=1, tiled=True),
        preferred_element_type=jnp.float32,
    )
    expo = jnp.exp(logits)
    probs = expo / jnp.sum(expo, axis=-1, keepdims=True)
    expert_ids = jnp.arange(experts, dtype=jnp.int32)
    picks = (routes[:, :, :, None] == expert_ids[None, None, None, :]).astype(jnp.float32)
    d_prob = jnp.sum(cotangent[:, :, :, None] * picks, axis=2)
    inner = jnp.sum(probs * d_prob, axis=-1, keepdims=True)
    d_logits = (probs * (d_prob - inner)).astype(jnp.bfloat16)
    batch_rows = lax.psum_scatter(
        jnp.einsum("ltd,lte->dle", acts, d_logits, preferred_element_type=jnp.float32),
        "batch",
        scatter_dimension=0,
        tiled=True,
    )
    summed = lax.psum_scatter(batch_rows, "seq", scatter_dimension=0, tiled=True)
    summed = jnp.transpose(summed, (1, 0, 2))
    square_sum = lax.psum(jnp.sum(summed * summed), ("batch", "seq", "section"))
    entry_count = 1.0 * layers * lax.axis_size("section") * width * experts
    clip_norm = 0.25 * math.sqrt(entry_count)
    clip_scale = jnp.minimum(jnp.float32(1.0), clip_norm / jnp.sqrt(square_sum))
    return summed * clip_scale


def kernel(cfg, acts_hbm, cot_hbm, routes_hbm, w_hbm, out_ref,
           acts_v, cot_ref, routes_ref, wq, wg, logit, dprob, dt, part, low, rec_c, rec_f, rec_s, rec_l, rec_h,
           quad, flip, sq,
           load_sem, q_send, q_recv, ag_send, ag_recv, fw_send, fw_recv,
           rs_send, rs_recv, fin_send, fin_recv, sq_send, sq_recv):
    n_batch, n_seq, tokens, width, experts, rows, chunks, clip_norm = cfg
    n_dev = n_batch * n_seq
    quad_cols = 4 * rows
    tail = experts - LANES
    half, quarter = experts // 2, experts // 4
    hrow = rows // 2
    b, s = lax.axis_index("batch"), lax.axis_index("seq")
    y, x = b // 2, b % 2
    z, c = s // 2, s % 2
    zh, zl = z // 2, z % 2
    me = b * n_seq + s
    p_own = zl * 2 + c

    def dev(dy=0, dx=0, dh=0, dl=0, dc=0):
        bb = ((y + dy) % 2) * 2 + (x + dx) % 2
        ss = (((zh + dh) % 2) * 2 + (zl + dl) % 2) * 2 + (c + dc) % 2
        return (bb, ss, 0)

    core, near, far = dev(dc=1), dev(dl=1), dev(dh=1)
    first = dev(dx=1 - c, dy=c)
    second = dev(dx=c, dy=1 - c)

    barrier = pltpu.get_barrier_semaphore()
    for target in (core, near, far, first, second):
        pl.semaphore_signal(barrier, inc=1, device_id=target, device_id_type=MESH)
    loads = [pltpu.make_async_copy(src, dst, load_sem.at[i]) for i, (src, dst) in enumerate((
        (w_hbm, wq.at[p_own]), (cot_hbm, cot_ref), (routes_hbm, routes_ref), (acts_hbm, acts_v)))]
    for load in loads:
        load.start()
    loads[0].wait()
    pl.semaphore_wait(barrier, 5)

    sends = []

    def remote(src, dst, ssem, rsem, target):
        copy = pltpu.make_async_remote_copy(
            src_ref=src, dst_ref=dst, send_sem=ssem, recv_sem=rsem,
            device_id=target, device_id_type=MESH)
        copy.start()
        sends.append(copy)
        return copy

    to_core = remote(wq.at[p_own], wq.at[p_own], q_send.at[0], q_recv.at[0], core)
    to_near = remote(wq.at[p_own], wq.at[p_own], q_send.at[1], q_recv.at[1], near)

    loads[1].wait()
    loads[2].wait()
    expert = lax.broadcasted_iota(jnp.int32, (experts, tokens), 0)
    total = jnp.zeros((experts, tokens), jnp.float32)
    for k in range(cot_ref.shape[0]):
        total += jnp.where(routes_ref[k] == expert, cot_ref[k], 0.0)
    dprob[...] = total

    to_near.wait_recv()
    p_near = (1 - zl) * 2 + c
    relay = remote(wq.at[p_near], wq.at[p_near], q_send.at[2], q_recv.at[2], core)
    to_core.wait_recv()
    relay.wait_recv()

    def slot(df, ds, dz):
        yy = (y + df * c + ds * (1 - c)) % 2
        xx = (x + df * (1 - c) + ds * c) % 2
        return yy * 4 + xx * 2 + (zh + dz) % 2

    own = slot(0, 0, 0)
    for h in range(2):
        rng = slice(h * hrow, (h + 1) * hrow)
        for p in range(4):
            wg[own, h, p] = wq[p, rng, :LANES]
        wg[own, h, 4] = jnp.concatenate([wq[p, rng, LANES:] for p in range(4)], axis=1)

    pieces = ((0, 2), (2, 3))

    def gather(src, dst, i, target):
        at = slot(*src)
        n = (dst[0] * 4 + dst[1] * 2 + dst[2]) * 2 + i
        ref = wg.at[at, c, pl.ds(*pieces[i])]
        return remote(ref, ref, ag_send.at[n], ag_recv.at[n], target)

    def fw(src, i):
        at = slot(*src)
        n = (src[0] * 4 + src[1] * 2 + src[2]) * 2 + i
        ref = wg.at[at, c, pl.ds(*pieces[i])]
        return remote(ref, ref, fw_send.at[n], fw_recv.at[n], core)

    seg = lax.broadcasted_iota(jnp.int32, (rows, LANES), 1) // tail

    def add_logits(src, fresh=False):
        g = slot(*src)
        a_part = jnp.concatenate([wg[g, h, p] for p in range(4) for h in range(2)], axis=0)
        packed = jnp.concatenate([wg[g, 0, 4], wg[g, 1, 4]], axis=0)
        b_part = jnp.concatenate(
            [jnp.where(seg == p, packed, jnp.zeros_like(packed)) for p in range(4)], axis=0)
        w_part = jnp.concatenate([a_part, b_part], axis=1)
        cols = pl.ds(pl.multiple_of(g * quad_cols, LANES), quad_cols)
        term = jnp.dot(acts_v[:, cols], w_part, preferred_element_type=jnp.float32)
        if fresh:
            logit[...] = term
        else:
            logit[...] += term

    got, given = {}, {}
    for i in range(2):
        for dst, target in (((0, 0, 1), far), ((1, 0, 0), first), ((0, 1, 0), second)):
            got[dst, i] = gather((0, 0, 0), dst, i, target)
    loads[3].wait()
    add_logits((0, 0, 0), fresh=True)

    def arrive(src, i, onward=()):
        got[src, i].wait_recv()
        for dst, target in onward:
            got[dst, i] = gather(src, dst, i, target)
        given[src, i] = fw(src, i)

    def join(src):
        for i in range(2):
            given[(src[1], src[0], src[2]), i].wait_recv()
        add_logits(src)

    for i in range(2):
        arrive((1, 0, 0), i, [((1, 1, 0), second)])
        arrive((0, 1, 0), i)
    for i in range(2):
        arrive((0, 0, 1), i, [((1, 0, 1), first), ((0, 1, 1), second)])
        arrive((1, 1, 0), i)
        if i == 0:
            join((1, 0, 0))
            join((0, 1, 0))
    arrive((1, 0, 1), 0, [((1, 1, 1), second)])
    arrive((0, 1, 1), 0)
    join((0, 0, 1))
    join((1, 1, 0))
    arrive((1, 0, 1), 1, [((1, 1, 1), second)])
    arrive((0, 1, 1), 1)
    arrive((1, 1, 1), 0)
    join((1, 0, 1))
    join((0, 1, 1))
    arrive((1, 1, 1), 1)
    join((1, 1, 1))

    pad = jnp.zeros((flip.shape[0] - tokens, LANES), jnp.float32)
    turned = [jnp.transpose(jnp.concatenate([logit[:, j:j + LANES], pad], axis=0))[:, :tokens] for j in (0, LANES)]
    folded = sum(turned[1][r * tail:(r + 1) * tail] for r in range(4))
    expo = jnp.exp(jnp.concatenate([turned[0], folded], axis=0))
    probs = expo / jnp.sum(expo, axis=0, keepdims=True)
    inner = jnp.sum(probs * dprob[...], axis=0, keepdims=True)
    dt[...] = (probs * (dprob[...] - inner)).astype(jnp.bfloat16)

    def compute(k0, nk):
        for g in range(8):
            gy, gx, gz = g // 4, g // 2 % 2, g % 2
            at = g * quad_cols + k0 * LANES
            value = jnp.dot(dt[...], acts_v[:, at:at + nk * LANES], preferred_element_type=jnp.float32)
            for kk in range(nk):
                for h in range(2):
                    f, e = (gx, gy) if h == 0 else (gy, gx)
                    for q in range(2):
                        r = h * half + q * quarter
                        part[k0 + kk, h, f, e, gz, q] = value[r:r + quarter, kk * LANES:(kk + 1) * LANES]

    fi = x * (1 - c) + y * c
    si = y * (1 - c) + x * c
    n_chunks = len(chunks)

    def rs_start(stage, i):
        k0, nk = chunks[i]
        ks = pl.ds(k0, nk)
        src, dst, target = [
            lambda: (part.at[ks, 1 - c], rec_c.at[ks], core),
            lambda: (low.at[ks], rec_f.at[ks], first),
            lambda: (part.at[ks, c, fi, 1 - si], rec_s.at[ks], second),
            lambda: (part.at[ks, c, fi, si, :, 1 - zl], rec_l.at[ks], near),
            lambda: (part.at[ks, c, fi, si, 1 - zh, zl], rec_h.at[ks], far),
        ][stage]()
        n = stage * n_chunks + i
        return remote(src, dst, rs_send.at[n], rs_recv.at[n], target)

    def rs_finish(stage, i, copy):
        copy.wait_recv()
        k0, nk = chunks[i]
        for k in range(k0, k0 + nk):
            if stage == 0:
                part[k, c, fi] += rec_c[k, fi]
                mail = part[k, c, 1 - fi] + rec_c[k, 1 - fi]
                low[k] = mail.reshape(low.shape[1:]).astype(jnp.bfloat16)
            elif stage == 1:
                part[k, c, fi] += rec_f[k].astype(jnp.float32).reshape(part.shape[3:])
            elif stage == 2:
                part[k, c, fi, si] += rec_s[k]
            elif stage == 3:
                for q in range(2):
                    part[k, c, fi, si, q, zl] += rec_l[k, q]
            else:
                part[k, c, fi, si, zh, zl] += rec_h[k]

    flying = {}
    for i in range(n_chunks):
        compute(*chunks[i])
        flying[0, i] = rs_start(0, i)
        if i > 0:
            rs_finish(0, i - 1, flying[0, i - 1])
            flying[1, i - 1] = rs_start(1, i - 1)
    rs_finish(0, n_chunks - 1, flying[0, n_chunks - 1])
    flying[1, n_chunks - 1] = rs_start(1, n_chunks - 1)
    for wave in range(n_chunks + 3):
        for stage in (1, 2, 3, 4):
            i = wave - (stage - 1)
            if 0 <= i < n_chunks:
                rs_finish(stage, i, flying[stage, i])
                if stage < 4:
                    flying[stage + 1, i] = rs_start(stage + 1, i)

    squares = jnp.zeros((quarter, LANES), jnp.float32)
    for k in range(quad_cols // LANES):
        v = part[k, c, fi, si, zh, zl]
        rec_h[k] = v
        squares += v * v
    sq[me] = jnp.broadcast_to(jnp.sum(squares).reshape(1, 1), (1, LANES))
    sq_copies = []
    for d in range(1, n_dev):
        t = (me + d) % n_dev
        sq_copies.append(pltpu.make_async_remote_copy(
            src_ref=sq.at[me], dst_ref=sq.at[me], send_sem=sq_send.at[d], recv_sem=sq_recv.at[d],
            device_id=(t // n_seq, t % n_seq, 0), device_id_type=MESH))
        sq_copies[-1].start()
    q_own = c * 2 + zl
    fins = []
    for n, (dl, dc) in enumerate(((1, 0), (1, 1), (0, 1))):
        p_to = ((zl + dl) % 2) * 2 + (c + dc) % 2
        fins.append(remote(rec_h.at[pl.ds(p_to, 2)], quad.at[q_own], fin_send.at[n], fin_recv.at[n],
                           dev(dl=dl, dc=dc)))
    quad[q_own] = rec_h[pl.ds(p_own, 2)]
    for copy in fins:
        copy.wait_recv()
    for j in range(2):
        block = jnp.concatenate([quad[q, j] for q in range(4)]
                                + [jnp.zeros((2 * LANES - experts, LANES), jnp.float32)], axis=0)
        flip[j * LANES:(j + 1) * LANES, :] = jnp.transpose(block)
    for copy in sq_copies:
        copy.wait()
    total_sq = jnp.sum(jnp.sum(sq[...], axis=0)) * (1.0 / LANES)
    clip_scale = jnp.minimum(jnp.float32(1.0), clip_norm / jnp.sqrt(jnp.full((1, 1), total_sq, jnp.float32)))
    mine = flip[pl.ds(pl.multiple_of(p_own * (rows - LANES), 8), rows), :]
    out_ref[...] = mine[:, :experts] * clip_scale
    for copy in sends:
        copy.wait_send()


def fused(mesh, acts, cotangent, routes, router_weight):
    n_batch, n_seq = mesh.shape["batch"], mesh.shape["seq"]
    layers, tokens, width = acts.shape
    rows, experts = router_weight.shape[1:]
    topk = routes.shape[2]
    quad_tiles = 4 * rows // LANES
    quarter = experts // 4
    chunks = tuple((k, min(2, quad_tiles - k)) for k in range(0, quad_tiles, 2))
    clip_norm = 0.25 * math.sqrt(1.0 * layers * width * experts)
    cfg = (n_batch, n_seq, tokens, width, experts, rows, chunks, clip_norm)
    f32, bf16 = jnp.float32, jnp.bfloat16

    def by_choice(array):
        return jnp.transpose(array, (2, 0, 1))

    dma = pltpu.SemaphoreType.DMA
    vmem = pl.BlockSpec(memory_space=pltpu.VMEM)
    padded = -(-tokens // LANES) * LANES
    n_dev = n_batch * n_seq
    n_rs = 5 * len(chunks)
    out = pl.pallas_call(
        functools.partial(kernel, cfg),
        out_shape=jax.ShapeDtypeStruct((rows, experts), f32),
        in_specs=[pl.BlockSpec(memory_space=pltpu.HBM)] * 4,
        out_specs=vmem,
        scratch_shapes=[
            pltpu.VMEM((tokens, width), bf16),
            pltpu.VMEM((topk, 1, tokens), f32),
            pltpu.VMEM((topk, 1, tokens), jnp.int32),
            pltpu.VMEM((4, rows, experts), bf16),
            pltpu.VMEM((8, 2, 5, rows // 2, LANES), bf16),
            pltpu.VMEM((tokens, 2 * LANES), f32),
            pltpu.VMEM((experts, tokens), f32),
            pltpu.VMEM((experts, tokens), bf16),
            pltpu.VMEM((quad_tiles, 2, 2, 2, 2, 2, quarter, LANES), f32),
            pltpu.VMEM((quad_tiles, 2, 2, experts // 2, LANES), bf16),
            pltpu.VMEM((quad_tiles, 2, 2, 2, 2, quarter, LANES), f32),
            pltpu.VMEM((quad_tiles, 2, 2, experts // 2, LANES), bf16),
            pltpu.VMEM((quad_tiles, 2, 2, quarter, LANES), f32),
            pltpu.VMEM((quad_tiles, 2, quarter, LANES), f32),
            pltpu.VMEM((quad_tiles, quarter, LANES), f32),
            pltpu.VMEM((4, 2, quarter, LANES), f32),
            pltpu.VMEM((padded, 2 * LANES), f32),
            pltpu.VMEM((n_dev, 1, LANES), f32),
            dma((4,)), dma((3,)), dma((3,)), dma((16,)), dma((16,)), dma((16,)), dma((16,)),
            dma((n_rs,)), dma((n_rs,)), dma((3,)), dma((3,)), dma((n_dev,)), dma((n_dev,)),
        ],
        compiler_params=pltpu.CompilerParams(
            collective_id=0, has_side_effects=True, vmem_limit_bytes=67_043_328),
        name="router_grad",
    )(acts[0], by_choice(cotangent), by_choice(routes), router_weight[0])
    return out[None]


def solution(mesh):
    spec = P("section", ("batch", "seq"), None)

    def step(acts, cotangent, routes, router_weight):
        rows, experts = router_weight.shape[1:]
        cube = (mesh.shape["batch"], mesh.shape["seq"], mesh.shape["section"]) == (4, 8, 1)
        dense = (acts.shape[0] == 1 and LANES < experts == rows and 4 * (experts - LANES) == LANES
                 and 4 * rows == 5 * LANES and acts.shape[1] % 16 == 0)
        if cube and dense:
            return fused(mesh, acts, cotangent, routes, router_weight)
        return shards(acts, cotangent, routes, router_weight)

    return jax.shard_map(step, mesh=mesh, in_specs=(spec,) * 4, out_specs=spec, check_vma=False)
```

```python
import functools
import math

import jax
import jax.numpy as jnp
from jax import lax
from jax.experimental import pallas as pl
from jax.experimental.pallas import tpu as pltpu
from jax.sharding import PartitionSpec as P

MESH = pl.DeviceIdType.MESH
LANES = 128


def shards(acts, cotangent, routes, router_weight):
    layers = acts.shape[0]
    width = acts.shape[2]
    experts = router_weight.shape[2]
    logits = jnp.einsum(
        "ltd,lde->lte",
        acts,
        lax.all_gather(router_weight, ("batch", "seq"), axis=1, tiled=True),
        preferred_element_type=jnp.float32,
    )
    expo = jnp.exp(logits)
    probs = expo / jnp.sum(expo, axis=-1, keepdims=True)
    expert_ids = jnp.arange(experts, dtype=jnp.int32)
    picks = (routes[:, :, :, None] == expert_ids[None, None, None, :]).astype(jnp.float32)
    d_prob = jnp.sum(cotangent[:, :, :, None] * picks, axis=2)
    inner = jnp.sum(probs * d_prob, axis=-1, keepdims=True)
    d_logits = (probs * (d_prob - inner)).astype(jnp.bfloat16)
    batch_rows = lax.psum_scatter(
        jnp.einsum("ltd,lte->dle", acts, d_logits, preferred_element_type=jnp.float32),
        "batch",
        scatter_dimension=0,
        tiled=True,
    )
    summed = lax.psum_scatter(batch_rows, "seq", scatter_dimension=0, tiled=True)
    summed = jnp.transpose(summed, (1, 0, 2))
    square_sum = lax.psum(jnp.sum(summed * summed), ("batch", "seq", "section"))
    entry_count = 1.0 * layers * lax.axis_size("section") * width * experts
    clip_norm = 0.25 * math.sqrt(entry_count)
    clip_scale = jnp.minimum(jnp.float32(1.0), clip_norm / jnp.sqrt(square_sum))
    return summed * clip_scale


def kernel(cfg, acts_hbm, cot_hbm, routes_hbm, w_hbm, out_ref,
           acts_v, cot_ref, routes_ref, w_own, wq, wg, logit, dprob, dt, part, low, rec_c, rec_f, rec_s, rec_l, rec_h,
           quad, flip, sq,
           load_sem, q_send, q_recv, ag_send, ag_recv, fw_send, fw_recv,
           rs_send, rs_recv, fin_send, fin_recv, sq_send, sq_recv):
    n_batch, n_seq, tokens, width, experts, rows, chunks, clip_norm = cfg
    n_dev = n_batch * n_seq
    quad_cols = 4 * rows
    tail = experts - LANES
    half, quarter = experts // 2, experts // 4
    hrow = rows // 2
    b, s = lax.axis_index("batch"), lax.axis_index("seq")
    y, x = b // 2, b % 2
    z, c = s // 2, s % 2
    zh, zl = z // 2, z % 2
    me = b * n_seq + s
    p_own = zl * 2 + c

    def dev(dy=0, dx=0, dh=0, dl=0, dc=0):
        bb = ((y + dy) % 2) * 2 + (x + dx) % 2
        ss = (((zh + dh) % 2) * 2 + (zl + dl) % 2) * 2 + (c + dc) % 2
        return (bb, ss, 0)

    core, near, far = dev(dc=1), dev(dl=1), dev(dh=1)
    first = dev(dx=1 - c, dy=c)
    second = dev(dx=c, dy=1 - c)

    barrier = pltpu.get_barrier_semaphore()
    for target in (core, near, dev(dl=1, dc=1), far, first, second):
        pl.semaphore_signal(barrier, inc=1, device_id=target, device_id_type=MESH)
    loads = [pltpu.make_async_copy(src, dst, load_sem.at[i]) for i, (src, dst) in enumerate((
        (w_hbm, w_own), (cot_hbm, cot_ref), (routes_hbm, routes_ref), (acts_hbm, acts_v)))]
    for load in loads:
        load.start()
    loads[0].wait()
    pl.semaphore_wait(barrier, 6)

    sends = []

    def remote(src, dst, ssem, rsem, target):
        copy = pltpu.make_async_remote_copy(
            src_ref=src, dst_ref=dst, send_sem=ssem, recv_sem=rsem,
            device_id=target, device_id_type=MESH)
        copy.start()
        sends.append(copy)
        return copy

    quad_in = []
    for n, (target, h) in enumerate(((near, c), (dev(dl=1, dc=1), 1 - c), (core, 1 - c))):
        quad_in.append(remote(w_own.at[h], wq.at[p_own], q_send.at[n], q_recv.at[n], target))
    wq[p_own] = w_own[c]

    loads[1].wait()
    loads[2].wait()
    expert = lax.broadcasted_iota(jnp.int32, (experts, tokens), 0)
    total = jnp.zeros((experts, tokens), jnp.float32)
    for k in range(cot_ref.shape[0]):
        total += jnp.where(routes_ref[k] == expert, cot_ref[k], 0.0)
    dprob[...] = total

    for copy in quad_in:
        copy.wait_recv()

    def slot(df, ds, dz):
        yy = (y + df * c + ds * (1 - c)) % 2
        xx = (x + df * (1 - c) + ds * c) % 2
        return yy * 4 + xx * 2 + (zh + dz) % 2

    own = slot(0, 0, 0)
    for p in range(4):
        wg[own, c, p] = wq[p, :, :LANES]
    wg[own, c, 4] = jnp.concatenate([wq[p, :, LANES:] for p in range(4)], axis=1)

    pieces = ((0, 2), (2, 2), (4, 1))
    n_pieces = len(pieces)

    def gather(src, dst, i, target):
        at = slot(*src)
        n = (dst[0] * 4 + dst[1] * 2 + dst[2]) * n_pieces + i
        ref = wg.at[at, c, pl.ds(*pieces[i])]
        return remote(ref, ref, ag_send.at[n], ag_recv.at[n], target)

    def fw(src, i):
        at = slot(*src)
        n = (src[0] * 4 + src[1] * 2 + src[2]) * n_pieces + i
        ref = wg.at[at, c, pl.ds(*pieces[i])]
        return remote(ref, ref, fw_send.at[n], fw_recv.at[n], core)

    seg = lax.broadcasted_iota(jnp.int32, (rows, LANES), 1) // tail

    def add_logits(src, fresh=False):
        g = slot(*src)
        a_part = jnp.concatenate([wg[g, h, p] for p in range(4) for h in range(2)], axis=0)
        packed = jnp.concatenate([wg[g, 0, 4], wg[g, 1, 4]], axis=0)
        b_part = jnp.concatenate(
            [jnp.where(seg == p, packed, jnp.zeros_like(packed)) for p in range(4)], axis=0)
        w_part = jnp.concatenate([a_part, b_part], axis=1)
        cols = pl.ds(pl.multiple_of(g * quad_cols, LANES), quad_cols)
        term = jnp.dot(acts_v[:, cols], w_part, preferred_element_type=jnp.float32)
        if fresh:
            logit[...] = term
        else:
            logit[...] += term

    got, given = {}, {}
    for i in range(n_pieces):
        for dst, target in (((0, 0, 1), far), ((1, 0, 0), first), ((0, 1, 0), second)):
            got[dst, i] = gather((0, 0, 0), dst, i, target)
        given[(0, 0, 0), i] = fw((0, 0, 0), i)
    loads[3].wait()

    def arrive(src, i, onward=()):
        got[src, i].wait_recv()
        for dst, target in onward:
            got[dst, i] = gather(src, dst, i, target)
        given[src, i] = fw(src, i)

    def join(src):
        for i in range(n_pieces):
            given[(src[1], src[0], src[2]), i].wait_recv()
        add_logits(src, fresh=src == (0, 0, 0))

    join((0, 0, 0))
    for i in range(n_pieces):
        arrive((1, 0, 0), i, [((1, 1, 0), second)])
        arrive((0, 1, 0), i)
    beyond = [((1, 0, 1), first), ((0, 1, 1), second)]
    arrive((0, 0, 1), 0, beyond)
    join((1, 0, 0))
    join((0, 1, 0))
    arrive((0, 0, 1), 1, beyond)
    arrive((1, 1, 0), 0)
    arrive((1, 0, 1), 0, [((1, 1, 1), second)])
    arrive((0, 0, 1), 2, beyond)
    arrive((1, 1, 0), 1)
    arrive((1, 1, 0), 2)
    arrive((1, 0, 1), 1, [((1, 1, 1), second)])
    join((0, 0, 1))
    join((1, 1, 0))
    arrive((1, 0, 1), 2, [((1, 1, 1), second)])
    for i in range(n_pieces):
        arrive((0, 1, 1), i)
    arrive((1, 1, 1), 0)
    arrive((1, 1, 1), 1)
    join((1, 0, 1))
    join((0, 1, 1))
    arrive((1, 1, 1), 2)
    join((1, 1, 1))

    pad = jnp.zeros((flip.shape[0] - tokens, LANES), jnp.float32)
    turned = [jnp.transpose(jnp.concatenate([logit[:, j:j + LANES], pad], axis=0))[:, :tokens] for j in (0, LANES)]
    folded = sum(turned[1][r * tail:(r + 1) * tail] for r in range(4))
    expo = jnp.exp(jnp.concatenate([turned[0], folded], axis=0))
    probs = expo / jnp.sum(expo, axis=0, keepdims=True)
    inner = jnp.sum(probs * dprob[...], axis=0, keepdims=True)
    dt[...] = (probs * (dprob[...] - inner)).astype(jnp.bfloat16)

    def compute(k0, nk):
        for g in range(8):
            gy, gx, gz = g // 4, g // 2 % 2, g % 2
            at = g * quad_cols + k0 * LANES
            value = jnp.dot(dt[...], acts_v[:, at:at + nk * LANES], preferred_element_type=jnp.float32)
            for kk in range(nk):
                for h in range(2):
                    f, e = (gx, gy) if h == 0 else (gy, gx)
                    for q in range(2):
                        r = h * half + q * quarter
                        part[k0 + kk, h, f, e, gz, q] = value[r:r + quarter, kk * LANES:(kk + 1) * LANES]

    fi = x * (1 - c) + y * c
    si = y * (1 - c) + x * c
    n_chunks = len(chunks)

    def rs_start(stage, i):
        k0, nk = chunks[i]
        ks = pl.ds(k0, nk)
        src, dst, target = [
            lambda: (part.at[ks, 1 - c], rec_c.at[ks], core),
            lambda: (low.at[ks], rec_f.at[ks], first),
            lambda: (part.at[ks, c, fi, 1 - si], rec_s.at[ks], second),
            lambda: (part.at[ks, c, fi, si, :, 1 - zl], rec_l.at[ks], near),
            lambda: (part.at[ks, c, fi, si, 1 - zh, zl], rec_h.at[ks], far),
        ][stage]()
        n = stage * n_chunks + i
        return remote(src, dst, rs_send.at[n], rs_recv.at[n], target)

    def rs_finish(stage, i, copy):
        copy.wait_recv()
        k0, nk = chunks[i]
        for k in range(k0, k0 + nk):
            if stage == 0:
                part[k, c, fi] += rec_c[k, fi]
                mail = part[k, c, 1 - fi] + rec_c[k, 1 - fi]
                low[k] = mail.reshape(low.shape[1:]).astype(jnp.bfloat16)
            elif stage == 1:
                part[k, c, fi] += rec_f[k].astype(jnp.float32).reshape(part.shape[3:])
            elif stage == 2:
                part[k, c, fi, si] += rec_s[k]
            elif stage == 3:
                for q in range(2):
                    part[k, c, fi, si, q, zl] += rec_l[k, q]
            else:
                part[k, c, fi, si, zh, zl] += rec_h[k]

    flying = {}
    for i in range(n_chunks):
        compute(*chunks[i])
        flying[0, i] = rs_start(0, i)
        if i > 0:
            rs_finish(0, i - 1, flying[0, i - 1])
            flying[1, i - 1] = rs_start(1, i - 1)
    rs_finish(0, n_chunks - 1, flying[0, n_chunks - 1])
    flying[1, n_chunks - 1] = rs_start(1, n_chunks - 1)
    for wave in range(n_chunks + 3):
        for stage in (1, 2, 3, 4):
            i = wave - (stage - 1)
            if 0 <= i < n_chunks:
                rs_finish(stage, i, flying[stage, i])
                if stage < 4:
                    flying[stage + 1, i] = rs_start(stage + 1, i)

    squares = jnp.zeros((quarter, LANES), jnp.float32)
    for k in range(quad_cols // LANES):
        v = part[k, c, fi, si, zh, zl]
        rec_h[k] = v
        squares += v * v
    sq[me] = jnp.broadcast_to(jnp.sum(squares).reshape(1, 1), (1, LANES))
    sq_copies = []
    for d in range(1, n_dev):
        t = (me + d) % n_dev
        sq_copies.append(pltpu.make_async_remote_copy(
            src_ref=sq.at[me], dst_ref=sq.at[me], send_sem=sq_send.at[d], recv_sem=sq_recv.at[d],
            device_id=(t // n_seq, t % n_seq, 0), device_id_type=MESH))
        sq_copies[-1].start()
    q_own = c * 2 + zl
    fins = []
    for n, (dl, dc) in enumerate(((1, 0), (1, 1), (0, 1))):
        p_to = ((zl + dl) % 2) * 2 + (c + dc) % 2
        fins.append(remote(rec_h.at[pl.ds(p_to, 2)], quad.at[q_own], fin_send.at[n], fin_recv.at[n],
                           dev(dl=dl, dc=dc)))
    quad[q_own] = rec_h[pl.ds(p_own, 2)]
    for copy in fins:
        copy.wait_recv()
    for j in range(2):
        block = jnp.concatenate([quad[q, j] for q in range(4)]
                                + [jnp.zeros((2 * LANES - experts, LANES), jnp.float32)], axis=0)
        flip[j * LANES:(j + 1) * LANES, :] = jnp.transpose(block)
    for copy in sq_copies:
        copy.wait()
    total_sq = jnp.sum(jnp.sum(sq[...], axis=0)) * (1.0 / LANES)
    clip_scale = jnp.minimum(jnp.float32(1.0), clip_norm / jnp.sqrt(jnp.full((1, 1), total_sq, jnp.float32)))
    mine = flip[pl.ds(pl.multiple_of(p_own * (rows - LANES), 8), rows), :]
    out_ref[...] = mine[:, :experts] * clip_scale
    for copy in sends:
        copy.wait_send()


def fused(mesh, acts, cotangent, routes, router_weight):
    n_batch, n_seq = mesh.shape["batch"], mesh.shape["seq"]
    layers, tokens, width = acts.shape
    rows, experts = router_weight.shape[1:]
    topk = routes.shape[2]
    quad_tiles = 4 * rows // LANES
    quarter = experts // 4
    chunks = tuple((k, min(2, quad_tiles - k)) for k in range(0, quad_tiles, 2))
    clip_norm = 0.25 * math.sqrt(1.0 * layers * width * experts)
    cfg = (n_batch, n_seq, tokens, width, experts, rows, chunks, clip_norm)
    f32, bf16 = jnp.float32, jnp.bfloat16

    def by_choice(array):
        return jnp.transpose(array, (2, 0, 1))

    dma = pltpu.SemaphoreType.DMA
    vmem = pl.BlockSpec(memory_space=pltpu.VMEM)
    padded = -(-tokens // LANES) * LANES
    n_dev = n_batch * n_seq
    n_rs = 5 * len(chunks)
    out = pl.pallas_call(
        functools.partial(kernel, cfg),
        out_shape=jax.ShapeDtypeStruct((rows, experts), f32),
        in_specs=[pl.BlockSpec(memory_space=pltpu.HBM)] * 4,
        out_specs=vmem,
        scratch_shapes=[
            pltpu.VMEM((tokens, width), bf16),
            pltpu.VMEM((topk, 1, tokens), f32),
            pltpu.VMEM((topk, 1, tokens), jnp.int32),
            pltpu.VMEM((2, rows // 2, experts), bf16),
            pltpu.VMEM((4, rows // 2, experts), bf16),
            pltpu.VMEM((8, 2, 5, rows // 2, LANES), bf16),
            pltpu.VMEM((tokens, 2 * LANES), f32),
            pltpu.VMEM((experts, tokens), f32),
            pltpu.VMEM((experts, tokens), bf16),
            pltpu.VMEM((quad_tiles, 2, 2, 2, 2, 2, quarter, LANES), f32),
            pltpu.VMEM((quad_tiles, 2, 2, experts // 2, LANES), bf16),
            pltpu.VMEM((quad_tiles, 2, 2, 2, 2, quarter, LANES), f32),
            pltpu.VMEM((quad_tiles, 2, 2, experts // 2, LANES), bf16),
            pltpu.VMEM((quad_tiles, 2, 2, quarter, LANES), f32),
            pltpu.VMEM((quad_tiles, 2, quarter, LANES), f32),
            pltpu.VMEM((quad_tiles, quarter, LANES), f32),
            pltpu.VMEM((4, 2, quarter, LANES), f32),
            pltpu.VMEM((padded, 2 * LANES), f32),
            pltpu.VMEM((n_dev, 1, LANES), f32),
            dma((4,)), dma((3,)), dma((3,)), dma((24,)), dma((24,)), dma((24,)), dma((24,)),
            dma((n_rs,)), dma((n_rs,)), dma((3,)), dma((3,)), dma((n_dev,)), dma((n_dev,)),
        ],
        compiler_params=pltpu.CompilerParams(
            collective_id=0, has_side_effects=True, vmem_limit_bytes=67_043_328),
        name="router_grad",
    )(acts[0], by_choice(cotangent), by_choice(routes), router_weight.reshape(2, rows // 2, experts))
    return out[None]


def solution(mesh):
    spec = P("section", ("batch", "seq"), None)

    def step(acts, cotangent, routes, router_weight):
        rows, experts = router_weight.shape[1:]
        cube = (mesh.shape["batch"], mesh.shape["seq"], mesh.shape["section"]) == (4, 8, 1)
        dense = (acts.shape[0] == 1 and LANES < experts == rows and 4 * (experts - LANES) == LANES
                 and 4 * rows == 5 * LANES and acts.shape[1] % 16 == 0)
        if cube and dense:
            return fused(mesh, acts, cotangent, routes, router_weight)
        return shards(acts, cotangent, routes, router_weight)

    return jax.shard_map(step, mesh=mesh, in_specs=(spec,) * 4, out_specs=spec, check_vma=False)
```

```python
import functools
import math

import jax
import jax.numpy as jnp
from jax import lax
from jax.experimental import pallas as pl
from jax.experimental.pallas import tpu as pltpu
from jax.sharding import PartitionSpec as P

MESH = pl.DeviceIdType.MESH
LANES = 128


def shards(acts, cotangent, routes, router_weight):
    layers = acts.shape[0]
    width = acts.shape[2]
    experts = router_weight.shape[2]
    logits = jnp.einsum(
        "ltd,lde->lte",
        acts,
        lax.all_gather(router_weight, ("batch", "seq"), axis=1, tiled=True),
        preferred_element_type=jnp.float32,
    )
    expo = jnp.exp(logits)
    probs = expo / jnp.sum(expo, axis=-1, keepdims=True)
    expert_ids = jnp.arange(experts, dtype=jnp.int32)
    picks = (routes[:, :, :, None] == expert_ids[None, None, None, :]).astype(jnp.float32)
    d_prob = jnp.sum(cotangent[:, :, :, None] * picks, axis=2)
    inner = jnp.sum(probs * d_prob, axis=-1, keepdims=True)
    d_logits = (probs * (d_prob - inner)).astype(jnp.bfloat16)
    batch_rows = lax.psum_scatter(
        jnp.einsum("ltd,lte->dle", acts, d_logits, preferred_element_type=jnp.float32),
        "batch",
        scatter_dimension=0,
        tiled=True,
    )
    summed = lax.psum_scatter(batch_rows, "seq", scatter_dimension=0, tiled=True)
    summed = jnp.transpose(summed, (1, 0, 2))
    square_sum = lax.psum(jnp.sum(summed * summed), ("batch", "seq", "section"))
    entry_count = 1.0 * layers * lax.axis_size("section") * width * experts
    clip_norm = 0.25 * math.sqrt(entry_count)
    clip_scale = jnp.minimum(jnp.float32(1.0), clip_norm / jnp.sqrt(square_sum))
    return summed * clip_scale


def kernel(cfg, acts_hbm, cot_hbm, routes_hbm, w_hbm, out_ref,
           acts_v, cot_ref, routes_ref, wq, wg, logit, dprob, dt, part, low, low_s, rec_t, rec_c, rec_f, rec_s, rec_l, rec_h,
           quad, flip, sq,
           load_sem, q_send, q_recv, ag_send, ag_recv, fw_send, fw_recv,
           rs_send, rs_recv, fin_send, fin_recv, sq_send, sq_recv):
    n_batch, n_seq, tokens, width, experts, rows, chunks, clip_norm = cfg
    n_dev = n_batch * n_seq
    quad_cols = 4 * rows
    tail = experts - LANES
    half, quarter = experts // 2, experts // 4
    hrow = rows // 2
    b, s = lax.axis_index("batch"), lax.axis_index("seq")
    y, x = b // 2, b % 2
    z, c = s // 2, s % 2
    zh, zl = z // 2, z % 2
    me = b * n_seq + s
    p_own = zl * 2 + c

    def dev(dy=0, dx=0, dh=0, dl=0, dc=0):
        bb = ((y + dy) % 2) * 2 + (x + dx) % 2
        ss = (((zh + dh) % 2) * 2 + (zl + dl) % 2) * 2 + (c + dc) % 2
        return (bb, ss, 0)

    core, near, far = dev(dc=1), dev(dl=1), dev(dh=1)
    first = dev(dx=1 - c, dy=c)
    second = dev(dx=c, dy=1 - c)

    barrier = pltpu.get_barrier_semaphore()
    for target in (core, near, far, first, second):
        pl.semaphore_signal(barrier, inc=1, device_id=target, device_id_type=MESH)
    loads = [pltpu.make_async_copy(src, dst, load_sem.at[i]) for i, (src, dst) in enumerate((
        (w_hbm, wq.at[p_own]), (cot_hbm, cot_ref), (routes_hbm, routes_ref), (acts_hbm, acts_v)))]
    for load in loads:
        load.start()
    loads[0].wait()
    pl.semaphore_wait(barrier, 5)

    sends = []

    def remote(src, dst, ssem, rsem, target):
        copy = pltpu.make_async_remote_copy(
            src_ref=src, dst_ref=dst, send_sem=ssem, recv_sem=rsem,
            device_id=target, device_id_type=MESH)
        copy.start()
        sends.append(copy)
        return copy

    to_core = remote(wq.at[p_own], wq.at[p_own], q_send.at[0], q_recv.at[0], core)
    to_near = remote(wq.at[p_own], wq.at[p_own], q_send.at[1], q_recv.at[1], near)

    loads[1].wait()
    loads[2].wait()
    expert = lax.broadcasted_iota(jnp.int32, (experts, tokens), 0)
    total = jnp.zeros((experts, tokens), jnp.float32)
    for k in range(cot_ref.shape[0]):
        total += jnp.where(routes_ref[k] == expert, cot_ref[k], 0.0)
    dprob[...] = total

    to_near.wait_recv()
    p_near = (1 - zl) * 2 + c
    relay = remote(wq.at[p_near], wq.at[p_near], q_send.at[2], q_recv.at[2], core)
    to_core.wait_recv()
    relay.wait_recv()

    def slot(df, ds, dz):
        yy = (y + df * c + ds * (1 - c)) % 2
        xx = (x + df * (1 - c) + ds * c) % 2
        return yy * 4 + xx * 2 + (zh + dz) % 2

    own = slot(0, 0, 0)
    for h in range(2):
        rng = slice(h * hrow, (h + 1) * hrow)
        for p in range(4):
            wg[own, h, p] = wq[p, rng, :LANES]
        wg[own, h, 4] = jnp.concatenate([wq[p, rng, LANES:] for p in range(4)], axis=1)

    pieces = ((0, 2), (2, 3))

    def gather(src, dst, i, target):
        at = slot(*src)
        n = (dst[0] * 4 + dst[1] * 2 + dst[2]) * 2 + i
        ref = wg.at[at, c, pl.ds(*pieces[i])]
        return remote(ref, ref, ag_send.at[n], ag_recv.at[n], target)

    def fw(src, i):
        at = slot(*src)
        n = (src[0] * 4 + src[1] * 2 + src[2]) * 2 + i
        ref = wg.at[at, c, pl.ds(*pieces[i])]
        return remote(ref, ref, fw_send.at[n], fw_recv.at[n], core)

    seg = lax.broadcasted_iota(jnp.int32, (rows, LANES), 1) // tail

    def add_logits(src, fresh=False):
        g = slot(*src)
        a_part = jnp.concatenate([wg[g, h, p] for p in range(4) for h in range(2)], axis=0)
        packed = jnp.concatenate([wg[g, 0, 4], wg[g, 1, 4]], axis=0)
        b_part = jnp.concatenate(
            [jnp.where(seg == p, packed, jnp.zeros_like(packed)) for p in range(4)], axis=0)
        w_part = jnp.concatenate([a_part, b_part], axis=1)
        cols = pl.ds(pl.multiple_of(g * quad_cols, LANES), quad_cols)
        term = jnp.dot(acts_v[:, cols], w_part, preferred_element_type=jnp.float32)
        if fresh:
            logit[...] = term
        else:
            logit[...] += term

    got, given = {}, {}
    for i in range(2):
        for dst, target in (((0, 0, 1), far), ((1, 0, 0), first), ((0, 1, 0), second)):
            got[dst, i] = gather((0, 0, 0), dst, i, target)
    loads[3].wait()
    add_logits((0, 0, 0), fresh=True)

    def arrive(src, i, onward=()):
        got[src, i].wait_recv()
        for dst, target in onward:
            got[dst, i] = gather(src, dst, i, target)
        given[src, i] = fw(src, i)

    def join(src):
        for i in range(2):
            given[(src[1], src[0], src[2]), i].wait_recv()
        add_logits(src)

    for i in range(2):
        arrive((1, 0, 0), i, [((1, 1, 0), second)])
        arrive((0, 1, 0), i)
    for i in range(2):
        arrive((0, 0, 1), i, [((1, 0, 1), first), ((0, 1, 1), second)])
        arrive((1, 1, 0), i)
        if i == 0:
            join((1, 0, 0))
            join((0, 1, 0))
    arrive((1, 0, 1), 0, [((1, 1, 1), second)])
    arrive((0, 1, 1), 0)
    join((0, 0, 1))
    join((1, 1, 0))
    arrive((1, 0, 1), 1, [((1, 1, 1), second)])
    arrive((0, 1, 1), 1)
    arrive((1, 1, 1), 0)
    join((1, 0, 1))
    join((0, 1, 1))
    arrive((1, 1, 1), 1)
    join((1, 1, 1))

    pad = jnp.zeros((flip.shape[0] - tokens, LANES), jnp.float32)
    turned = [jnp.transpose(jnp.concatenate([logit[:, j:j + LANES], pad], axis=0))[:, :tokens] for j in (0, LANES)]
    folded = sum(turned[1][r * tail:(r + 1) * tail] for r in range(4))
    expo = jnp.exp(jnp.concatenate([turned[0], folded], axis=0))
    probs = expo / jnp.sum(expo, axis=0, keepdims=True)
    inner = jnp.sum(probs * dprob[...], axis=0, keepdims=True)
    dt[...] = (probs * (dprob[...] - inner)).astype(jnp.bfloat16)

    def compute(k0, nk):
        for g in range(8):
            gy, gx, gz = g // 4, g // 2 % 2, g % 2
            at = g * quad_cols + k0 * LANES
            value = jnp.dot(dt[...], acts_v[:, at:at + nk * LANES], preferred_element_type=jnp.float32)
            for kk in range(nk):
                for h in range(2):
                    f, e = (gx, gy) if h == 0 else (gy, gx)
                    for q in range(2):
                        r = h * half + q * quarter
                        part[k0 + kk, h, f, e, gz, q] = value[r:r + quarter, kk * LANES:(kk + 1) * LANES]

    fi = x * (1 - c) + y * c
    si = y * (1 - c) + x * c
    n_chunks = len(chunks)

    def rs_start(stage, i):
        k0, nk = chunks[i]
        ks = pl.ds(k0, nk)
        src, dst, target = [
            lambda: (part.at[ks, 1 - c], rec_c.at[ks], core),
            lambda: (low.at[ks], rec_f.at[ks], first),
            lambda: (low_s.at[ks], rec_t.at[ks], second) if i == 0 else (part.at[ks, c, fi, 1 - si], rec_s.at[ks], second),
            lambda: (part.at[ks, c, fi, si, :, 1 - zl], rec_l.at[ks], near),
            lambda: (part.at[ks, c, fi, si, 1 - zh, zl], rec_h.at[ks], far),
        ][stage]()
        n = stage * n_chunks + i
        return remote(src, dst, rs_send.at[n], rs_recv.at[n], target)

    def rs_finish(stage, i, copy):
        copy.wait_recv()
        k0, nk = chunks[i]
        for k in range(k0, k0 + nk):
            if stage == 0:
                part[k, c, fi] += rec_c[k, fi]
                mail = part[k, c, 1 - fi] + rec_c[k, 1 - fi]
                low[k] = mail.reshape(low.shape[1:]).astype(jnp.bfloat16)
            elif stage == 1:
                part[k, c, fi] += rec_f[k].astype(jnp.float32).reshape(part.shape[3:])
                if i == 0:
                    low_s[k] = part[k, c, fi, 1 - si].reshape(low_s.shape[1:]).astype(jnp.bfloat16)
            elif stage == 2:
                if i == 0:
                    part[k, c, fi, si] += rec_t[k].astype(jnp.float32).reshape(part.shape[4:])
                else:
                    part[k, c, fi, si] += rec_s[k]
            elif stage == 3:
                for q in range(2):
                    part[k, c, fi, si, q, zl] += rec_l[k, q]
            else:
                part[k, c, fi, si, zh, zl] += rec_h[k]

    flying = {}
    for i in range(n_chunks):
        compute(*chunks[i])
        flying[0, i] = rs_start(0, i)
        if i > 0:
            rs_finish(0, i - 1, flying[0, i - 1])
            flying[1, i - 1] = rs_start(1, i - 1)
    rs_finish(0, n_chunks - 1, flying[0, n_chunks - 1])
    flying[1, n_chunks - 1] = rs_start(1, n_chunks - 1)
    for wave in range(n_chunks + 3):
        for stage in (1, 2, 3, 4):
            i = wave - (stage - 1)
            if 0 <= i < n_chunks:
                rs_finish(stage, i, flying[stage, i])
                if stage < 4:
                    flying[stage + 1, i] = rs_start(stage + 1, i)

    squares = jnp.zeros((quarter, LANES), jnp.float32)
    for k in range(quad_cols // LANES):
        v = part[k, c, fi, si, zh, zl]
        rec_h[k] = v
        squares += v * v
    sq[me] = jnp.broadcast_to(jnp.sum(squares).reshape(1, 1), (1, LANES))
    sq_copies = []
    for d in range(1, n_dev):
        t = (me + d) % n_dev
        sq_copies.append(pltpu.make_async_remote_copy(
            src_ref=sq.at[me], dst_ref=sq.at[me], send_sem=sq_send.at[d], recv_sem=sq_recv.at[d],
            device_id=(t // n_seq, t % n_seq, 0), device_id_type=MESH))
        sq_copies[-1].start()
    q_own = c * 2 + zl
    fins = []
    for n, (dl, dc) in enumerate(((1, 0), (1, 1), (0, 1))):
        p_to = ((zl + dl) % 2) * 2 + (c + dc) % 2
        fins.append(remote(rec_h.at[pl.ds(p_to, 2)], quad.at[q_own], fin_send.at[n], fin_recv.at[n],
                           dev(dl=dl, dc=dc)))
    quad[q_own] = rec_h[pl.ds(p_own, 2)]
    for copy in fins:
        copy.wait_recv()
    for j in range(2):
        block = jnp.concatenate([quad[q, j] for q in range(4)]
                                + [jnp.zeros((2 * LANES - experts, LANES), jnp.float32)], axis=0)
        flip[j * LANES:(j + 1) * LANES, :] = jnp.transpose(block)
    for copy in sq_copies:
        copy.wait()
    total_sq = jnp.sum(jnp.sum(sq[...], axis=0)) * (1.0 / LANES)
    clip_scale = jnp.minimum(jnp.float32(1.0), clip_norm / jnp.sqrt(jnp.full((1, 1), total_sq, jnp.float32)))
    mine = flip[pl.ds(pl.multiple_of(p_own * (rows - LANES), 8), rows), :]
    out_ref[...] = mine[:, :experts] * clip_scale
    for copy in sends:
        copy.wait_send()


def fused(mesh, acts, cotangent, routes, router_weight):
    n_batch, n_seq = mesh.shape["batch"], mesh.shape["seq"]
    layers, tokens, width = acts.shape
    rows, experts = router_weight.shape[1:]
    topk = routes.shape[2]
    quad_tiles = 4 * rows // LANES
    quarter = experts // 4
    chunks = tuple((k, min(2, quad_tiles - k)) for k in range(0, quad_tiles, 2))
    clip_norm = 0.25 * math.sqrt(1.0 * layers * width * experts)
    cfg = (n_batch, n_seq, tokens, width, experts, rows, chunks, clip_norm)
    f32, bf16 = jnp.float32, jnp.bfloat16

    def by_choice(array):
        return jnp.transpose(array, (2, 0, 1))

    dma = pltpu.SemaphoreType.DMA
    vmem = pl.BlockSpec(memory_space=pltpu.VMEM)
    padded = -(-tokens // LANES) * LANES
    n_dev = n_batch * n_seq
    n_rs = 5 * len(chunks)
    out = pl.pallas_call(
        functools.partial(kernel, cfg),
        out_shape=jax.ShapeDtypeStruct((rows, experts), f32),
        in_specs=[pl.BlockSpec(memory_space=pltpu.HBM)] * 4,
        out_specs=vmem,
        scratch_shapes=[
            pltpu.VMEM((tokens, width), bf16),
            pltpu.VMEM((topk, 1, tokens), f32),
            pltpu.VMEM((topk, 1, tokens), jnp.int32),
            pltpu.VMEM((4, rows, experts), bf16),
            pltpu.VMEM((8, 2, 5, rows // 2, LANES), bf16),
            pltpu.VMEM((tokens, 2 * LANES), f32),
            pltpu.VMEM((experts, tokens), f32),
            pltpu.VMEM((experts, tokens), bf16),
            pltpu.VMEM((quad_tiles, 2, 2, 2, 2, 2, quarter, LANES), f32),
            pltpu.VMEM((quad_tiles, 2, 2, experts // 2, LANES), bf16),
            pltpu.VMEM((chunks[0][1], 2, experts // 2, LANES), bf16),
            pltpu.VMEM((chunks[0][1], 2, experts // 2, LANES), bf16),
            pltpu.VMEM((quad_tiles, 2, 2, 2, 2, quarter, LANES), f32),
            pltpu.VMEM((quad_tiles, 2, 2, experts // 2, LANES), bf16),
            pltpu.VMEM((quad_tiles, 2, 2, quarter, LANES), f32),
            pltpu.VMEM((quad_tiles, 2, quarter, LANES), f32),
            pltpu.VMEM((quad_tiles, quarter, LANES), f32),
            pltpu.VMEM((4, 2, quarter, LANES), f32),
            pltpu.VMEM((padded, 2 * LANES), f32),
            pltpu.VMEM((n_dev, 1, LANES), f32),
            dma((4,)), dma((3,)), dma((3,)), dma((16,)), dma((16,)), dma((16,)), dma((16,)),
            dma((n_rs,)), dma((n_rs,)), dma((3,)), dma((3,)), dma((n_dev,)), dma((n_dev,)),
        ],
        compiler_params=pltpu.CompilerParams(
            collective_id=0, has_side_effects=True, vmem_limit_bytes=67_043_328),
        name="router_grad",
    )(acts[0], by_choice(cotangent), by_choice(routes), router_weight[0])
    return out[None]


def solution(mesh):
    spec = P("section", ("batch", "seq"), None)

    def step(acts, cotangent, routes, router_weight):
        rows, experts = router_weight.shape[1:]
        cube = (mesh.shape["batch"], mesh.shape["seq"], mesh.shape["section"]) == (4, 8, 1)
        dense = (acts.shape[0] == 1 and LANES < experts == rows and 4 * (experts - LANES) == LANES
                 and 4 * rows == 5 * LANES and acts.shape[1] % 16 == 0)
        if cube and dense:
            return fused(mesh, acts, cotangent, routes, router_weight)
        return shards(acts, cotangent, routes, router_weight)

    return jax.shard_map(step, mesh=mesh, in_specs=(spec,) * 4, out_specs=spec, check_vma=False)
```
